32 devices in a mesh: region: 8 (over z, y), sub: 4 (over x, core).
Axes of the slice: x: 2, y: 2, z: 4, core: 2. Of those that a mesh axis runs over, the one named last changes fastest.
Arguments:
- density: bfloat16 [8, 4, 192, 2048], P('region', 'sub'), may hold values from -6 to 6
- inverse: bfloat16 [8, 4, 2048, 2048], P('region', 'sub'), may hold values from -0.125 to 0.125
- projection: bfloat16 [8, 4, 2048, 256], P('region', 'sub'), may hold values from -0.125 to 0.125
- points: float32 [8, 4, 3, 2048], P('region'), may hold values from 0 to 1
- skeleton_points: float32 [8, 4, 3, 256], replicated, may hold values from 0 to 1
- neighbours: int32 [8, 4, 2], P('region', 'sub'), may hold values from 0 to 3, as said below
- reads: int32 [8, 16, 2], replicated, may hold values from 0 to 7, as said below
Outputs:
- result: bfloat16 [8, 4, 192, 2048], P('region', 'sub')
The draws below stay inside these ranges and needn't reach their ends.
Inputs may be any that keep to these rules, and one draw needn't show every extreme that they name: `neighbours`: each subdomain lists 2 distinct other subdomains of its own region. In reads[g], entries c * 4 to (c + 1) * 4 - 1 have block index // 2 equal to c; their owner regions are distinct and differ from g.
All inputs are finite; a program needn't handle non-finite values.
Results may differ from the reference program's by a relative error of at most 0.0067.
Values may be sent and summed in bfloat16 or wider, within the bound.
A program may use at most 128 MiB of HBM per device.

```python
import jax
import jax.numpy as jnp
from jax import lax

ORDER = 2048
RIGHT_SIDES = 192
SKEL_RANK = 256
BLOCK_ROWS = 128
MATES_LISTED = 2
REGIONS = 8
REGION_SUBS = 4
BLOCKS_EACH = 2
PER_COLUMN = 4
LIST_LENGTH = 16


def draw_neighbours(key, part):
    scores = jax.random.randint(key, (REGIONS, REGION_SUBS, REGION_SUBS), 0, 65536) * REGION_SUBS + jnp.arange(REGION_SUBS, dtype=jnp.int32)
    same_index = jnp.arange(REGION_SUBS)[:, None] == jnp.arange(REGION_SUBS)[None, :]
    scores = jnp.where(same_index[None], -1, scores)
    return lax.top_k(scores, MATES_LISTED)[1].astype(jnp.int32)


def draw_reads(key, part):
    hot_key = jax.random.fold_in(key, 11)
    base_key = jax.random.fold_in(key, 12)
    half_key = jax.random.fold_in(key, 13)
    hotness = jax.random.randint(hot_key, (REGIONS,), 0, 4) * 65536
    base_scores = jax.random.randint(base_key, (REGIONS, REGION_SUBS, REGIONS), 0, 65536)
    scores = (base_scores + hotness[None, None, :]) * REGIONS + jnp.arange(REGIONS, dtype=jnp.int32)
    reader_self = jnp.arange(REGIONS)[:, None, None] == jnp.arange(REGIONS)[None, None, :]
    scores = jnp.where(reader_self, -1, scores)
    owners = lax.top_k(scores, PER_COLUMN)[1].astype(jnp.int32)
    halves = jax.random.randint(half_key, (REGIONS, REGION_SUBS, PER_COLUMN), 0, BLOCKS_EACH)
    blocks = jnp.arange(REGION_SUBS, dtype=jnp.int32)[None, :, None] * BLOCKS_EACH + halves
    return jnp.stack([owners, blocks.astype(jnp.int32)], axis=-1).reshape(REGIONS, LIST_LENGTH, 2).astype(jnp.int32)


def block_scale(key, dims, shards, smallest, top_value):
    factor_of = 1.0
    for dim, shards_of in shards:
        steps = jax.random.uniform(jax.random.fold_in(jax.random.fold_in(key, 6), dim), (shards_of,), jnp.float32, smallest / len(shards), top_value / len(shards))
        factor_of = factor_of * jnp.repeat(jnp.exp(steps), dims[dim] // shards_of).reshape((-1,) + (1,) * (len(dims) - 1 - dim))
    return factor_of


def centred(stream_key, shape, spread, most, pieces=(), kind=jnp.bfloat16):
    loudness = block_scale(stream_key, shape, pieces, -0.22, 0.18) if pieces else 1.0
    array = jax.random.normal(stream_key, shape, jnp.float32) * spread * loudness
    return jnp.minimum(jnp.maximum(array, -most), most).astype(kind)


def setup_inputs(seed: int = 0) -> dict:
    streams_of = jax.random.split(jax.random.key(seed), 8)
    return {
        "density": centred(streams_of[0], (REGIONS, REGION_SUBS, RIGHT_SIDES, ORDER), 1.0, 6.0, ((0, 8), (1, 4))),
        "inverse": centred(streams_of[1], (REGIONS, REGION_SUBS, ORDER, ORDER), ORDER ** -0.5, 0.125, ((0, 8), (1, 4))),
        "projection": centred(streams_of[2], (REGIONS, REGION_SUBS, ORDER, SKEL_RANK), ORDER ** -0.5, 0.125, ((0, 8), (1, 4))),
        "points": jnp.clip(1.0 * jax.random.uniform(streams_of[3], (REGIONS, REGION_SUBS, 3, ORDER), jnp.float32) ** block_scale(streams_of[3], (REGIONS, REGION_SUBS, 3, ORDER), ((0, 8),), -0.2, 0.2), 0.0, 1.0),
        "skeleton_points": jnp.clip(jax.random.uniform(streams_of[4], (REGIONS, REGION_SUBS, 3, SKEL_RANK), jnp.float32, 0.0, 1.0), 0.0, 1.0),
        "neighbours": draw_neighbours(jax.random.fold_in(streams_of[7], 71), 0),
        "reads": draw_reads(jax.random.fold_in(streams_of[7], 71), 0),
    }


damping = 1.0
softening = 0.05

def kernel(source, target):
    apart_x = source[0][:, None] - target[0][None, :]
    apart_y = source[1][:, None] - target[1][None, :]
    apart_z = source[2][:, None] - target[2][None, :]
    squared = apart_x * apart_x + apart_y * apart_y + apart_z * apart_z
    kernel_tiles = jnp.exp(-damping * jnp.sqrt(squared)) / jnp.sqrt(squared + softening * softening)
    return (kernel_tiles * target.shape[1] ** (-0.5)).astype(jnp.bfloat16)

def product_pair(operands):
    return jnp.dot(operands[0], operands[1], preferred_element_type=jnp.float32).astype(jnp.bfloat16)

def reference(density, inverse, projection, points, skeleton_points, neighbours, reads):
    devices_all = REGIONS * REGION_SUBS
    flat_rhs = density.reshape(devices_all, RIGHT_SIDES, ORDER)
    flat_inverse = inverse.reshape(devices_all, ORDER, ORDER)
    flat_projection = projection.reshape(devices_all, ORDER, SKEL_RANK)
    solved = lax.map(product_pair, (flat_rhs, flat_inverse))
    strengths = lax.map(product_pair, (solved, flat_projection))
    blocks_each = SKEL_RANK // BLOCK_ROWS
    block_points = skeleton_points.reshape(devices_all, 3, blocks_each, BLOCK_ROWS)
    block_strengths = strengths.reshape(devices_all, RIGHT_SIDES, blocks_each, BLOCK_ROWS)

    def one_device(device):
        region = device // REGION_SUBS
        member = device % REGION_SUBS
        own_points = points[region, member]
        near_field = jnp.zeros((RIGHT_SIDES, ORDER), jnp.float32)
        for position in range(MATES_LISTED):
            mate_index = neighbours[region, member, position]
            coupling = kernel(points[region, mate_index], own_points)
            near_field = near_field + jnp.dot(solved[region * REGION_SUBS + mate_index], coupling, preferred_element_type=jnp.float32)
        entries = reads[region]
        owner_devices = (entries[:, 0] * REGION_SUBS + entries[:, 1] // blocks_each).astype(jnp.int32)
        halves = (entries[:, 1] % blocks_each).astype(jnp.int32)
        chosen = jnp.take_along_axis(block_strengths[owner_devices], halves[:, None, None, None], axis=2)[:, :, 0]
        located = jnp.take_along_axis(block_points[owner_devices], halves[:, None, None, None], axis=2)[:, :, 0]
        values = jnp.transpose(chosen, (1, 0, 2)).reshape(RIGHT_SIDES, LIST_LENGTH * BLOCK_ROWS)
        sources = jnp.transpose(located, (1, 0, 2)).reshape(3, LIST_LENGTH * BLOCK_ROWS)
        far_field = jnp.dot(values, kernel(sources, own_points), preferred_element_type=jnp.float32)
        applied = (flat_rhs[device].astype(jnp.float32) + near_field + far_field).astype(jnp.bfloat16)
        return jnp.dot(applied, flat_inverse[device], preferred_element_type=jnp.float32).astype(jnp.bfloat16)
    result = lax.map(one_device, jnp.arange(devices_all, dtype=jnp.int32))
    return result.reshape(REGIONS, REGION_SUBS, RIGHT_SIDES, ORDER)
```

```python
import functools

import jax
import jax.numpy as jnp
from jax import lax
from jax.experimental import pallas as pl
from jax.experimental.pallas import tpu as pltpu
from jax.sharding import PartitionSpec as P

BLOCK_ROWS = 128
DAMPING = 1.0
SOFTENING = 0.05
LOG2E = 1.4426950408889634
FACTOR = DAMPING * LOG2E
FLOOR = 1e-30
TERMS = 24
ROWS = 256
PIECES = 4
MESH = pl.DeviceIdType.MESH
f32, bf16 = jnp.float32, jnp.bfloat16


def split(x):
    a = x.astype(bf16).astype(f32)
    b = (x - a).astype(bf16).astype(f32)
    c = (x - a - b).astype(bf16).astype(f32)
    return a, b, c


def prepared(coords):
    u = (coords - 0.5) * FACTOR
    norm = jnp.sum(u * u, axis=0, keepdims=True)
    return split(u), split(norm)


def fill_source(dst, coords, start):
    (a, b, c), (k, l, m) = prepared(coords)
    cols = pl.ds(start, coords.shape[1])
    for i, part in enumerate((a, a, b, b, a, c)):
        dst[3 * i : 3 * i + 3, cols] = part
    dst[18:19, cols] = k
    dst[19:20, cols] = l
    dst[20:21, cols] = m
    dst[21:24, cols] = jnp.ones((3, coords.shape[1]), f32)


def fill_target(dst, coords):
    (a, b, c), (k, l, m) = prepared(coords)
    for i, part in enumerate((a, b, a, b, c, a)):
        dst[3 * i : 3 * i + 3, :] = -2.0 * part
    dst[18:21, :] = jnp.ones((3, coords.shape[1]), f32)
    dst[21:22, :] = k
    dst[22:23, :] = l
    dst[23:24, :] = m


def body(n, regions, per_column, blocks_each,
         neighbours, reads, density, inverse, projection, points, skeleton,
         out,
         inv, near_k, far_k, shards, picked, arrived, outgoing, strengths, applied, total,
         source, target, far_source,
         inv_sem, x_send, x_recv, d_send, d_recv, f_send, f_recv,
         a_send, a_recv, px_send, px_recv, pd_send, pd_recv, pf_send, pf_recv):
    sub = lax.axis_index("sub")
    region = lax.axis_index("region")
    order = inv.shape[0]
    width = order // PIECES
    half = n // 2
    peer = sub + 1 - 2 * lax.rem(sub, 2)

    for p in range(PIECES):
        cols = pl.ds(p * width, width)
        pltpu.make_async_copy(inverse.at[0, 0, :, cols], inv.at[:, cols], inv_sem.at[p]).start()

    barrier = pltpu.get_barrier_semaphore()
    for k in range(1, n):
        pl.semaphore_signal(barrier, inc=1, device_id={"sub": lax.rem(sub + k, n)}, device_id_type=MESH)
    for k in range(1, regions):
        pl.semaphore_signal(barrier, inc=1, device_id={"region": lax.rem(region + k, regions)}, device_id_type=MESH)

    def remote(ref, dev, send, recv):
        return pltpu.make_async_remote_copy(
            src_ref=ref, dst_ref=ref, send_sem=send, recv_sem=recv, device_id=dev, device_id_type=MESH
        )

    def same(k):
        return lax.rem(sub + 2 * k, n)

    def origin(who, k):
        return lax.rem(who - 2 * k + n, n)

    def piece(o, p):
        return shards.at[o, :, pl.ds(p * width, width)]

    fill_target(target, points[0, sub])

    def send_piece(p):
        for k in range(1, half):
            remote(piece(sub, p), {"sub": same(k)}, x_send.at[k, p], x_recv.at[k, p]).start()
        remote(piece(sub, p), {"sub": peer}, d_send.at[p], d_recv.at[p]).start()

    for p in range(PIECES):
        cols = pl.ds(p * width, width)
        pltpu.make_async_copy(inverse.at[0, 0, :, cols], inv.at[:, cols], inv_sem.at[p]).wait()
        shards[sub, :, cols] = jnp.dot(
            density[0, 0], inv[:, cols], preferred_element_type=f32
        ).astype(bf16)
        if p == 0:
            pl.semaphore_wait(barrier, n - 1 + regions - 1)
        else:
            send_piece(p - 1)
    strengths[...] = jnp.dot(shards[sub], projection[0, 0], preferred_element_type=f32).astype(bf16)
    send_piece(PIECES - 1)

    def wanted(r):
        which = jnp.int32(0)
        for j in range(per_column):
            at = (r * per_column * n + sub * per_column + j) * 2
            which = which + jnp.where(reads[at] == region, lax.rem(reads[at + 1], blocks_each), 0)
        return which

    def pick_half(value, which):
        chosen = value[:, :BLOCK_ROWS]
        for b in range(1, blocks_each):
            chosen = jnp.where(which == b, value[:, b * BLOCK_ROWS : (b + 1) * BLOCK_ROWS], chosen)
        return chosen

    def exchange(k):
        return pltpu.make_async_remote_copy(
            src_ref=outgoing.at[k - 1], dst_ref=arrived.at[k - 1],
            send_sem=a_send.at[k], recv_sem=a_recv.at[k],
            device_id={"region": lax.rem(region + k, regions)}, device_id_type=MESH,
        )

    def prepare_out(k, _):
        outgoing[k - 1] = pick_half(strengths[...], wanted(lax.rem(region + k, regions)))
        return 0

    lax.fori_loop(1, regions, prepare_out, 0)

    def start_out(k, _):
        exchange(k).start()
        return 0

    lax.fori_loop(1, regions, start_out, 0)

    def generate(src, base, dst, rows):
        def step(i, _):
            at = pl.multiple_of(i * ROWS, ROWS)
            a = src[:, pl.ds(pl.multiple_of(base + at, ROWS), ROWS)].astype(bf16)
            for j in range(order // 256):
                b = target[:, j * 256 : (j + 1) * 256].astype(bf16)
                d2 = lax.dot_general(a, b, (((0,), (0,)), ((), ())), preferred_element_type=f32)
                d2 = jnp.maximum(d2.astype(bf16), jnp.array(FLOOR, bf16))
                decay = jnp.exp2(-(d2 * lax.rsqrt(d2)))
                soft = lax.rsqrt(d2 + jnp.array((FACTOR * SOFTENING) ** 2, bf16))
                dst[pl.ds(at, ROWS), j * 256 : (j + 1) * 256] = decay * soft
            return 0

        lax.fori_loop(0, rows // ROWS, step, 0)

    def forward(p):
        for k in range(1, half):
            o = origin(sub, k)
            remote(piece(o, p), {"sub": peer}, x_send.at[k, p], x_recv.at[k, p]).wait_recv()
            remote(piece(o, p), {"sub": peer}, f_send.at[k, p], f_recv.at[k, p]).start()

    mates = near_k.shape[0]
    p = 0
    for m in range(mates):
        fill_source(source, points[0, neighbours[m]], 0)
        generate(source, 0, near_k.at[m], order)
        if p < PIECES - 1:
            forward(p)
            p += 1

    def wait_out(k, _):
        exchange(k).wait_recv()
        return 0

    lax.fori_loop(1, regions, wait_out, 0)
    for j in range(per_column):
        at = ((region * n + sub) * per_column + j) * 2
        slot = jnp.maximum(lax.rem(region - reads[at] + regions, regions) - 1, 0)
        picked[sub, :, j * BLOCK_ROWS : (j + 1) * BLOCK_ROWS] = arrived[slot]

    far_w = per_column * BLOCK_ROWS
    for e in range(n * per_column):
        at = (region * n * per_column + e) * 2
        blk = reads[at + 1]
        located = skeleton[reads[at], lax.div(blk, blocks_each)]
        fill_source(far_source, pick_half(located, lax.rem(blk, blocks_each)), e * BLOCK_ROWS)

    for k in range(1, half):
        remote(picked.at[sub], {"sub": same(k)}, px_send.at[k], px_recv.at[k]).start()
    remote(picked.at[sub], {"sub": peer}, pd_send, pd_recv).start()

    ready = far_k.shape[0] // far_w
    generate(far_source, 0, far_k, far_k.shape[0])
    while p < PIECES:
        forward(p)
        p += 1
    for p in range(PIECES):
        remote(piece(peer, p), {"sub": peer}, d_send.at[p], d_recv.at[p]).wait_recv()
        for k in range(1, half):
            remote(piece(origin(peer, k), p), {"sub": peer}, f_send.at[k, p], f_recv.at[k, p]).wait_recv()

    tiles = order // width

    def near_tile(t, _):
        cols = pl.ds(pl.multiple_of(t * width, width), width)
        acc = jnp.dot(shards[neighbours[0]], near_k[0, :, cols], preferred_element_type=f32)
        for m in range(1, mates):
            acc += jnp.dot(shards[neighbours[m]], near_k[m, :, cols], preferred_element_type=f32)
        total[:, cols] = acc
        return 0

    lax.fori_loop(0, tiles, near_tile, 0)

    for k in range(1, half):
        o = origin(sub, k)
        remote(picked.at[o], {"sub": peer}, px_send.at[k], px_recv.at[k]).wait_recv()
        remote(picked.at[o], {"sub": peer}, pf_send.at[k], pf_recv.at[k]).start()
    remote(picked.at[peer], {"sub": peer}, pd_send, pd_recv).wait_recv()
    for k in range(1, half):
        remote(picked.at[origin(peer, k)], {"sub": peer}, pf_send.at[k], pf_recv.at[k]).wait_recv()

    for c in range(ready, n):
        generate(far_source, c * far_w, near_k.at[0], far_w)

        def more(t, _):
            cols = pl.ds(pl.multiple_of(t * width, width), width)
            total[:, cols] += jnp.dot(picked[c], near_k[0, :far_w, cols], preferred_element_type=f32)
            return 0

        lax.fori_loop(0, tiles, more, 0)

    scale = FACTOR * order ** -0.5

    def far_tile(t, _):
        cols = pl.ds(pl.multiple_of(t * width, width), width)
        acc = total[:, cols]
        for c in range(ready):
            acc += jnp.dot(
                picked[c], far_k[c * far_w : (c + 1) * far_w, cols], preferred_element_type=f32
            )
        applied[:, cols] = (density[0, 0, :, cols].astype(f32) + scale * acc).astype(bf16)
        return 0

    lax.fori_loop(0, tiles, far_tile, 0)

    def result_tile(t, _):
        cols = pl.ds(pl.multiple_of(t * width, width), width)
        out[0, 0, :, cols] = jnp.dot(
            applied[...], inv[:, cols], preferred_element_type=f32
        ).astype(bf16)
        return 0

    lax.fori_loop(0, tiles, result_tile, 0)

    def drain(k, _):
        exchange(k).wait_send()
        return 0

    lax.fori_loop(1, regions, drain, 0)
    for p in range(PIECES):
        remote(piece(sub, p), {"sub": peer}, d_send.at[p], d_recv.at[p]).wait_send()
        for k in range(1, half):
            remote(piece(sub, p), {"sub": same(k)}, x_send.at[k, p], x_recv.at[k, p]).wait_send()
            remote(piece(origin(sub, k), p), {"sub": peer}, f_send.at[k, p], f_recv.at[k, p]).wait_send()
    remote(picked.at[sub], {"sub": peer}, pd_send, pd_recv).wait_send()
    for k in range(1, half):
        remote(picked.at[sub], {"sub": same(k)}, px_send.at[k], px_recv.at[k]).wait_send()
        remote(picked.at[origin(sub, k)], {"sub": peer}, pf_send.at[k], pf_recv.at[k]).wait_send()


def per_device(density, inverse, projection, points, skeleton_points, neighbours, reads):
    n = lax.axis_size("sub")
    regions = lax.axis_size("region")
    _, _, rows, order = density.shape
    rank = projection.shape[3]
    blocks_each = rank // BLOCK_ROWS
    per_column = reads.shape[1] // n
    mates = neighbours.shape[2]
    far_w = per_column * BLOCK_ROWS
    ready = min(n, max(1, order // far_w))
    half = n // 2
    dma = pltpu.SemaphoreType.DMA
    vmem = pl.BlockSpec(memory_space=pltpu.VMEM)
    smem = pl.BlockSpec(memory_space=pltpu.SMEM)
    return pl.pallas_call(
        functools.partial(body, n, regions, per_column, blocks_each),
        out_shape=jax.ShapeDtypeStruct(density.shape, bf16),
        in_specs=[smem, smem, vmem, pl.BlockSpec(memory_space=pl.ANY), vmem, vmem, vmem],
        out_specs=vmem,
        scratch_shapes=[
            pltpu.VMEM((order, order), bf16),
            pltpu.VMEM((mates, order, order), bf16),
            pltpu.VMEM((ready * far_w, order), bf16),
            pltpu.VMEM((n, rows, order), bf16),
            pltpu.VMEM((n, rows, far_w), bf16),
            pltpu.VMEM((regions - 1, rows, BLOCK_ROWS), bf16),
            pltpu.VMEM((regions - 1, rows, BLOCK_ROWS), bf16),
            pltpu.VMEM((rows, rank), bf16),
            pltpu.VMEM((rows, order), bf16),
            pltpu.VMEM((rows, order), f32),
            pltpu.VMEM((TERMS, order), f32),
            pltpu.VMEM((TERMS, order), f32),
            pltpu.VMEM((TERMS, n * far_w), f32),
            dma((PIECES,)),
            dma((half, PIECES)), dma((half, PIECES)),
            dma((PIECES,)), dma((PIECES,)),
            dma((half, PIECES)), dma((half, PIECES)),
            dma((regions,)), dma((regions,)),
            dma((half,)), dma((half,)),
            dma, dma,
            dma((half,)), dma((half,)),
        ],
        compiler_params=pltpu.CompilerParams(
            collective_id=0, has_side_effects=True, vmem_limit_bytes=60 * 1024 * 1024
        ),
    )(neighbours.reshape(-1), reads.reshape(-1), density, inverse, projection, points, skeleton_points)


def solution(mesh):
    return jax.shard_map(
        per_device,
        mesh=mesh,
        in_specs=(
            P("region", "sub", None, None),
            P("region", "sub", None, None),
            P("region", "sub", None, None),
            P("region", None, None, None),
            P(),
            P("region", "sub", None),
            P(),
        ),
        out_specs=P("region", "sub", None, None),
        check_vma=False,
    )
```
